16 devices in a mesh: dpy: 2 (over z), dpx: 2 (over y), tp: 4 (over x, core).
Axes of the slice: x: 2, y: 2, z: 2, core: 2. Of those that a mesh axis runs over, the one named last changes fastest.
Arguments:
- x_saved: bfloat16 [2, 32, 512, 2048], P(None, ('dpy', 'dpx'))
- y_saved: bfloat16 [2, 32, 512, 2048], P(None, ('dpy', 'dpx'))
- d_out: bfloat16 [32, 512, 2048], P(('dpy', 'dpx'))
- w_qkv: bfloat16 [2, 2048, 3, 32, 64], P(None, None, None, 'tp')
- w_out: bfloat16 [2, 32, 64, 2048], P(None, 'tp')
- w_up: bfloat16 [2, 2048, 8192], P(None, None, 'tp')
- w_down: bfloat16 [2, 8192, 2048], P(None, 'tp')
Outputs:
- output 1: bfloat16 [32, 512, 2048], P(('dpy', 'dpx'))
- output 2: float32 [2, 2048, 3, 32, 64], P(None, None, None, 'tp')
- output 3: float32 [2, 32, 64, 2048], P(None, 'tp')
- output 4: float32 [2, 2048, 8192], P(None, None, 'tp')
- output 5: float32 [2, 8192, 2048], P(None, 'tp')
All inputs are finite; a program needn't handle non-finite values.
Results may differ from the reference program's by a relative error of at most 0.02.
Values are sent between devices in bfloat16 or wider.
A program may use at most 1 GiB of HBM per device.

```python
import jax
import jax.numpy as jnp
from jax import lax

WIDTH = 2048
FFN = 8192
HEADS = 32
BATCH = 8
SEQ = 512
REPLICAS = 4
LAYERS = 2
HEAD_DIM = WIDTH // HEADS
SEQ_TOTAL = REPLICAS * BATCH


def setup_inputs(seed: int = 0) -> dict:
    root_key = jax.random.key(seed)
    sub_keys = jax.random.split(root_key, 7)
    act_shape = (LAYERS, SEQ_TOTAL, SEQ, WIDTH)
    x_saved = jax.random.normal(sub_keys[0], act_shape, jnp.float32).astype(jnp.bfloat16)
    y_saved = jax.random.normal(sub_keys[1], act_shape, jnp.float32).astype(jnp.bfloat16)
    d_out = jax.random.normal(sub_keys[2], (SEQ_TOTAL, SEQ, WIDTH), jnp.float32).astype(jnp.bfloat16)
    w_qkv = (jax.random.normal(sub_keys[3], (LAYERS, WIDTH, 3, HEADS, HEAD_DIM), jnp.float32) * WIDTH ** -0.5).astype(jnp.bfloat16)
    w_out = (jax.random.normal(sub_keys[4], (LAYERS, HEADS, HEAD_DIM, WIDTH), jnp.float32) * (4.0 * WIDTH ** -0.5)).astype(jnp.bfloat16)
    w_up = (jax.random.normal(sub_keys[5], (LAYERS, WIDTH, FFN), jnp.float32) * WIDTH ** -0.5).astype(jnp.bfloat16)
    w_down = (jax.random.normal(sub_keys[6], (LAYERS, FFN, WIDTH), jnp.float32) * (2.0 * FFN ** -0.5)).astype(jnp.bfloat16)
    return {'x_saved': x_saved, 'y_saved': y_saved, 'd_out': d_out, 'w_qkv': w_qkv, 'w_out': w_out, 'w_up': w_up, 'w_down': w_down}


def attention_backward(qkv_seq, d_att):
    queries = qkv_seq[:, 0].astype(jnp.float32)
    keys_all = qkv_seq[:, 1].astype(jnp.float32)
    values = qkv_seq[:, 2].astype(jnp.float32)
    datt_f32 = d_att.astype(jnp.float32)
    scale_factor = HEAD_DIM ** -0.5
    scores = jnp.einsum('qnd,knd->nqk', queries, keys_all) * scale_factor
    probs_f = jax.nn.softmax(scores, axis=-1)
    probs_b = probs_f.astype(jnp.bfloat16).astype(jnp.float32)
    att_out = jnp.einsum('nqk,knd->qnd', probs_b, values).astype(jnp.bfloat16)
    d_probs = jnp.einsum('qnd,knd->nqk', datt_f32, values)
    d_values = jnp.einsum('nqk,qnd->knd', probs_b, datt_f32).astype(jnp.bfloat16)
    row_dot = jnp.sum(d_probs * probs_f, axis=-1, keepdims=True)
    d_scores = (probs_f * (d_probs - row_dot) * scale_factor).astype(jnp.bfloat16).astype(jnp.float32)
    d_queries = jnp.einsum('nqk,knd->qnd', d_scores, keys_all).astype(jnp.bfloat16)
    d_keys = jnp.einsum('nqk,qnd->knd', d_scores, queries).astype(jnp.bfloat16)
    return att_out, jnp.stack([d_queries, d_keys, d_values], axis=1)


def layer_backward(x_in, y_mid, grad_out, wqkv_l, wout_l, wup_l, wdown_l):
    mid_f32 = y_mid.astype(jnp.float32)
    gout_f32 = grad_out.astype(jnp.float32)
    wup_f32 = wup_l.astype(jnp.float32)
    hidden = jnp.einsum('bsh,hf->bsf', mid_f32, wup_f32)
    act_f32, gelu_pull = jax.vjp(jax.nn.gelu, hidden)
    act_b = act_f32.astype(jnp.bfloat16).astype(jnp.float32)
    g_down = jnp.einsum('bsf,bsh->fh', act_b, gout_f32)
    d_act = jnp.einsum('bsh,fh->bsf', gout_f32, wdown_l.astype(jnp.float32))
    d_hidden = gelu_pull(d_act)[0].astype(jnp.bfloat16).astype(jnp.float32)
    g_up = jnp.einsum('bsh,bsf->hf', mid_f32, d_hidden)
    d_mid = (gout_f32 + jnp.einsum('bsf,hf->bsh', d_hidden, wup_f32)).astype(jnp.bfloat16)
    in_f32 = x_in.astype(jnp.float32)
    wqkv_f32 = wqkv_l.astype(jnp.float32)
    qkv = jnp.einsum('bsh,hcnd->bscnd', in_f32, wqkv_f32).astype(jnp.bfloat16)
    dmid_f32 = d_mid.astype(jnp.float32)
    d_att = jnp.einsum('bsh,ndh->bsnd', dmid_f32, wout_l.astype(jnp.float32)).astype(jnp.bfloat16)
    att_out, d_qkv = lax.map(lambda seq_pair: attention_backward(seq_pair[0], seq_pair[1]), (qkv, d_att))
    g_out = jnp.einsum('bsnd,bsh->ndh', att_out.astype(jnp.float32), dmid_f32)
    dqkv_f32 = d_qkv.astype(jnp.float32)
    g_qkv = jnp.einsum('bsh,bscnd->hcnd', in_f32, dqkv_f32)
    d_in = (dmid_f32 + jnp.einsum('bscnd,hcnd->bsh', dqkv_f32, wqkv_f32)).astype(jnp.bfloat16)
    return d_in, (g_qkv, g_out, g_up, g_down)


def reference(x_saved, y_saved, d_out, w_qkv, w_out, w_up, w_down):
    def replica_step(grad_sums, rep_idx):
        row_start = rep_idx * BATCH
        grad_cur = lax.dynamic_slice_in_dim(d_out, row_start, BATCH, axis=0)
        layer_grads = [None] * LAYERS
        for layer_idx in reversed(range(LAYERS)):
            x_in = lax.dynamic_slice_in_dim(x_saved[layer_idx], row_start, BATCH, axis=0)
            y_mid = lax.dynamic_slice_in_dim(y_saved[layer_idx], row_start, BATCH, axis=0)
            grad_cur, layer_grads[layer_idx] = layer_backward(x_in, y_mid, grad_cur, w_qkv[layer_idx], w_out[layer_idx], w_up[layer_idx], w_down[layer_idx])
        new_sums = tuple(sum_prev + jnp.stack([grad_set[slot_idx] for grad_set in layer_grads]) for slot_idx, sum_prev in enumerate(grad_sums))
        return new_sums, grad_cur

    init_sums = tuple(jnp.zeros(weight.shape, jnp.float32) for weight in (w_qkv, w_out, w_up, w_down))
    grad_sums, d_inputs = lax.scan(replica_step, init_sums, jnp.arange(REPLICAS))
    d_input = d_inputs.reshape(SEQ_TOTAL, SEQ, WIDTH)
    g_qkv, g_out, g_up, g_down = (sum_all / REPLICAS for sum_all in grad_sums)
    return d_input, g_qkv, g_out, g_up, g_down
```

```python
import jax
import jax.numpy as jnp
from jax import lax
from jax.experimental import pallas as pl
from jax.experimental.pallas import tpu as pltpu
from jax.sharding import PartitionSpec as P

MICROBATCHES = 2
LOG2E = 1.4426950408889634
F32 = jnp.float32
BF16 = jnp.bfloat16


def dot_f32(lhs, rhs, lhs_dim, rhs_dim):
    return lax.dot_general(lhs, rhs, (((lhs_dim,), (rhs_dim,)), ((), ())), preferred_element_type=F32)


def attention_body(heads_per_step, scale_factor, q_ref, k_ref, v_ref, datt_ref, out_ref, dqkv_ref):
    for head in range(heads_per_step):
        queries = q_ref[0, head]
        keys_all = k_ref[0, head]
        values = v_ref[0, head]
        d_att = datt_ref[0, head]
        scores = dot_f32(keys_all.T, queries, 1, 0)
        exps = jnp.exp2((scores - jnp.max(scores, axis=0, keepdims=True)) * (scale_factor * LOG2E))
        probs_f = exps * (1.0 / jnp.sum(exps, axis=0, keepdims=True))
        probs_b = probs_f.astype(BF16)
        out_ref[0, head] = dot_f32(values, probs_b, 1, 0).astype(BF16)
        d_probs = dot_f32(values.T, d_att, 1, 0)
        dqkv_ref[0, 2, head] = dot_f32(d_att, probs_b, 1, 1).astype(BF16)
        row_dot = jnp.sum(d_probs * probs_f, axis=0, keepdims=True)
        d_scores = (probs_f * (d_probs - row_dot) * scale_factor).astype(BF16)
        dqkv_ref[0, 0, head] = dot_f32(keys_all, d_scores, 1, 0).astype(BF16)
        dqkv_ref[0, 1, head] = dot_f32(queries, d_scores, 1, 1).astype(BF16)


def attention_backward(q_t, k_t, v_t, datt_t):
    batch, heads, head_dim, seq = datt_t.shape
    step = 2 if heads % 2 == 0 else 1
    flops = 12 * batch * heads * head_dim * seq * seq * 4

    def body(*refs):
        attention_body(step, head_dim ** -0.5, *refs)

    qkv_spec = pl.BlockSpec((1, 3, step, head_dim, seq), lambda b, n: (b, 0, n, 0, 0))
    att_spec = pl.BlockSpec((1, step, head_dim, seq), lambda b, n: (b, n, 0, 0))
    return pl.pallas_call(
        body,
        grid=(batch, heads // step),
        in_specs=[att_spec] * 4,
        out_specs=[att_spec, qkv_spec],
        out_shape=[jax.ShapeDtypeStruct(datt_t.shape, BF16), jax.ShapeDtypeStruct((batch, 3, heads, head_dim, seq), BF16)],
        cost_estimate=pl.CostEstimate(flops=flops, bytes_accessed=16 * datt_t.size, transcendentals=batch * heads * seq * seq),
        name='attn_bwd',
    )(q_t, k_t, v_t, datt_t)


def solution(mesh):
    data_axes = ('dpy', 'dpx')
    replicas = mesh.shape['dpy'] * mesh.shape['dpx']
    act_spec = P(None, data_axes, None, None)
    tok_spec = P(data_axes, None, None)
    qkv_spec = P(None, None, None, 'tp', None)
    wout_spec = P(None, 'tp', None, None)
    up_spec = P(None, None, 'tp')
    down_spec = P(None, 'tp', None)
    tp_size = mesh.shape['tp']
    core_swap = [(i, i ^ 1) for i in range(tp_size)]
    chip_swap = [(i, i ^ 2) for i in range(tp_size)]
    pair_swap = [(0, 1), (1, 0)]

    def pick(arr, index, axis):
        return lax.dynamic_index_in_dim(arr, index, axis, keepdims=False)

    def after(values, *earlier):
        tied = lax.optimization_barrier((tuple(values), tuple(earlier)))
        return tied[0]

    def tp_sum_half(part, residual, offset, *earlier):
        core = lax.rem(lax.axis_index('tp'), 2)
        half = part.shape[0] // 2
        res_half = lax.dynamic_slice_in_dim(residual, offset + core * half, half, 0)
        from_core = lax.ppermute(lax.dynamic_slice_in_dim(part, (1 - core) * half, half, 0), 'tp', core_swap)
        own = lax.dynamic_slice_in_dim(part, core * half, half, 0)
        chip_sum = (own.astype(F32) + from_core.astype(F32)).astype(BF16)
        from_chip, = after((lax.ppermute(chip_sum, 'tp', chip_swap),), *earlier)
        mine = (res_half.astype(F32) + (chip_sum.astype(F32) + from_chip.astype(F32))).astype(BF16)
        return mine, lax.ppermute(mine, 'tp', core_swap), chip_sum

    def join_halves(mine, other, _):
        core = lax.rem(lax.axis_index('tp'), 2)
        is_mine = (jnp.arange(2) == core)[:, None, None, None]
        both = jnp.where(is_mine, mine[None], other[None])
        return both.reshape((2 * mine.shape[0],) + mine.shape[1:])

    class ReplicaMean:
        def __init__(self, grad):
            self.rows, self.cols = grad.shape
            self.idx_y, self.idx_x = lax.axis_index('dpy'), lax.axis_index('dpx')
            self.blocks = grad.reshape(2, 2, 2, self.rows // 8, self.cols)
            self.sends = (self.cut(0, 1 - self.idx_x, 0, 2, 1).astype(BF16), self.cut(1 - self.idx_y, 0, 1, 1, 2).astype(BF16))
            self.recvs = (lax.ppermute(self.sends[0], 'dpx', pair_swap), lax.ppermute(self.sends[1], 'dpy', pair_swap))

        def cut(self, pos_y, pos_x, half, size_y, size_x):
            size = self.rows // 8
            out = lax.dynamic_slice(self.blocks, (pos_y, pos_x, half, 0, 0), (size_y, size_x, 1, size, self.cols))
            return out.reshape(size_y * size_x * size, self.cols)

        def part(self, recv, index):
            size = self.rows // 8
            return lax.dynamic_slice_in_dim(recv, index * size, size, 0).astype(F32)

        def second(self, *earlier):
            idx_y, idx_x = self.idx_y, self.idx_x
            recvs = self.recvs = after(self.recvs, *earlier)
            self.sends = ((self.cut(1 - idx_y, idx_x, 0, 1, 1) + self.part(recvs[0], 1 - idx_y)).astype(BF16),
                          (self.cut(idx_y, 1 - idx_x, 1, 1, 1) + self.part(recvs[1], 1 - idx_x)).astype(BF16))
            self.lasts = (lax.ppermute(self.sends[0], 'dpy', pair_swap), lax.ppermute(self.sends[1], 'dpx', pair_swap))
            return self.sends

        def third(self, *earlier):
            idx_y, idx_x = self.idx_y, self.idx_x
            lasts = after(self.lasts, *earlier)
            sum_first = self.cut(idx_y, idx_x, 0, 1, 1) + self.part(self.recvs[0], idx_y) + lasts[0].astype(F32)
            sum_second = self.cut(idx_y, idx_x, 1, 1, 1) + self.part(self.recvs[1], idx_x) + lasts[1].astype(F32)
            self.mine = (jnp.concatenate([sum_first, sum_second], axis=0) / replicas).astype(BF16)
            return self.mine

        def gathered(self):
            return lax.all_gather(self.mine, data_axes, axis=0, tiled=True).astype(F32)

    def device_backward(x_saved, y_saved, d_out, w_qkv, w_out, w_up, w_down):
        num_layers, width, _, heads, head_dim = w_qkv.shape
        cols = heads * head_dim
        rows = d_out.shape[0] // MICROBATCHES
        seq = d_out.shape[1]
        micro = [slice(i * rows, (i + 1) * rows) for i in range(MICROBATCHES)]
        grads = [d_out[m] for m in micro]
        sources = [(d_out, i * rows) for i in range(MICROBATCHES)]
        outs = [None] * 4
        pending = []
        upper = {}

        def mlp_down(hidden, grad):
            return jnp.einsum('bsf,bsh->fh', jax.nn.gelu(hidden).astype(BF16), grad, preferred_element_type=F32)

        def place(layer, slots, means):
            for slot, mean in zip(slots, means):
                block = mean.gathered()[None]
                if layer == num_layers - 1:
                    edge = ((0, 0, 0), (0, 0, 0))
                    outs[slot] = lax.pad(block, jnp.zeros((), F32), ((layer, 0, 0), *edge))
                else:
                    outs[slot] = lax.dynamic_update_slice(outs[slot], block, (layer, 0, 0))

        def mlp_data(layer, hidden, grad):
            _, gelu_pull = jax.vjp(jax.nn.gelu, hidden)
            d_act = jnp.einsum('bsh,fh->bsf', grad, w_down[layer], preferred_element_type=F32)
            d_hidden = gelu_pull(d_act)[0].astype(BF16)
            return d_hidden, jnp.einsum('bsf,hf->bsh', d_hidden, w_up[layer], preferred_element_type=F32).astype(BF16)

        for layer in reversed(range(num_layers)):
            wqkv_t = w_qkv[layer].transpose(1, 2, 3, 0).reshape(3 * cols, width)
            wout_l = w_out[layer].reshape(cols, width)
            hid = [jnp.einsum('bsh,hf->bsf', y_saved[layer, m], w_up[layer], preferred_element_type=F32) for m in micro]
            g_down = mlp_down(hid[0], grads[0])
            sends = [s for mean in pending for s in mean.second(g_down)]
            g_down = g_down + mlp_down(after((hid[1],), g_down, *sends)[0], grads[1])
            edges = [mean.third(g_down) for mean in pending]
            down = ReplicaMean(g_down)
            if layer < num_layers - 1:
                place(layer + 1, (2, 3), upper['mlp'])
                tied = after((hid[0], *outs[2:]), *down.sends, *edges)
                hid_0, outs[2:] = tied[0], tied[1:]
            else:
                hid_0, = after((hid[0],), *down.sends)
            d_hid_0, mid_0 = mlp_data(layer, hid_0, grads[0])
            mid_halves = [tp_sum_half(mid_0, *sources[0])]
            sends = down.second(mid_0)
            d_hid_1, mid_1 = mlp_data(layer, after((hid[1],), mid_0, mid_halves[0][2], *sends)[0], grads[1])
            mid_halves.append(tp_sum_half(mid_1, *sources[1], mid_halves[0][0]))
            mine = down.third(mid_1)
            d_hid_0, = after((d_hid_0,), mid_1, mine)
            g_up = jnp.einsum('bsh,bsf->hf', y_saved[layer, micro[0]], d_hid_0, preferred_element_type=F32)
            d_hid_1, = after((d_hid_1,), g_up, mid_halves[1][2])
            g_up += jnp.einsum('bsh,bsf->hf', y_saved[layer, micro[1]], d_hid_1, preferred_element_type=F32)
            up = ReplicaMean(g_up)
            edges = list(up.sends)
            if layer < num_layers - 1:
                place(layer + 1, (0, 1), upper['att'])
            mids, halves, out_ts, dqkv_ts = [], [], [], []
            for i, m in enumerate(micro):
                x_in = x_saved[layer, m]
                d_mid = join_halves(*after(mid_halves[i], *edges))
                if i == 0 and layer < num_layers - 1:
                    d_mid, *outs[:2] = after((d_mid, *outs[:2]))
                else:
                    d_mid, = after((d_mid,))
                qkv_t = [jnp.einsum('jh,bsh->bjs', wqkv_t[c * cols:(c + 1) * cols], x_in, preferred_element_type=F32).astype(BF16) for c in range(3)]
                datt_t = jnp.einsum('jh,bsh->bjs', wout_l, d_mid, preferred_element_type=F32).astype(BF16)
                out_t, dqkv_t = attention_backward(*[t.reshape(rows, heads, head_dim, seq) for t in (*qkv_t, datt_t)])
                dqkv_t = dqkv_t.reshape(rows, 3 * cols, seq)
                if i == 0:
                    dqkv_t, = after((dqkv_t,), *up.second(out_t))
                elif layer == 0:
                    dqkv_t, g_qkv = after((dqkv_t, g_qkv))
                    g_qkv += jnp.einsum('bjs,bsh->jh', dqkv_t, x_in, preferred_element_type=F32)
                    qkv_mean = ReplicaMean(g_qkv)
                    dqkv_t, = after((dqkv_t,), *qkv_mean.sends)
                in_part = jnp.einsum('bjs,jh->bsh', dqkv_t, wqkv_t, preferred_element_type=F32).astype(BF16)
                halves.append(tp_sum_half(in_part, d_mid, 0, *[half[0] for half in halves]))
                if i == 0:
                    edges = [in_part, halves[0][2], up.third(in_part)]
                    if layer == 0:
                        g_qkv = jnp.einsum('bjs,bsh->jh', after((dqkv_t,), in_part)[0], x_in, preferred_element_type=F32)
                        edges.append(g_qkv)
                mids.append(d_mid)
                out_ts.append(out_t.reshape(rows, cols, seq))
                dqkv_ts.append(dqkv_t)
            if layer > 0:
                dqkv_0, = after((dqkv_ts[0],), in_part)
                g_qkv = jnp.einsum('bjs,bsh->jh', dqkv_0, x_saved[layer, micro[0]], preferred_element_type=F32)
                dqkv_1, = after((dqkv_ts[1],), g_qkv, halves[1][2])
                g_qkv += jnp.einsum('bjs,bsh->jh', dqkv_1, x_saved[layer, micro[1]], preferred_element_type=F32)
                qkv_mean = ReplicaMean(g_qkv)
            out_ts = after(out_ts, in_part, halves[1][2], *qkv_mean.sends)
            g_out = sum(jnp.einsum('bjs,bsh->jh', out_ts[i], mids[i], preferred_element_type=F32) for i in range(MICROBATCHES))
            out_mean = ReplicaMean(g_out)
            upper = {'mlp': (up, down), 'att': (qkv_mean, out_mean)}
            if layer > 0:
                pending = [qkv_mean, out_mean]
                grad_0, = after((join_halves(*after(halves[0], in_part)),), *qkv_mean.sends, *out_mean.sends)
                grads = [grad_0, after((join_halves(*after(halves[1], grad_0)),))[0]]
                sources = [(g, 0) for g in grads]
        place(0, (2, 3), upper['mlp'])
        outs[2:] = after(outs[2:])
        for mean in upper['att']:
            mean.second(outs[2])
            mean.third()
        place(0, (0, 1), upper['att'])
        core = lax.rem(lax.axis_index('tp'), 2)
        d_in = lax.pad(join_halves(*after(halves[0], in_part)), jnp.zeros((), BF16), ((0, rows, 0), (0, 0, 0), (0, 0, 0)))
        mine, other, _ = halves[1]
        half = mine.shape[0]
        d_in = lax.dynamic_update_slice_in_dim(d_in, mine, rows + core * half, 0)
        d_in = lax.dynamic_update_slice_in_dim(d_in, other, rows + (1 - core) * half, 0)
        g_qkv = outs[0].reshape(num_layers, 3, heads, head_dim, width).transpose(0, 4, 1, 2, 3)
        g_out = outs[1].reshape(num_layers, heads, head_dim, width)
        return d_in, g_qkv, g_out, outs[2], outs[3]

    return jax.shard_map(device_backward, mesh=mesh, in_specs=(act_spec, act_spec, tok_spec, qkv_spec, wout_spec, up_spec, down_spec), out_specs=(tok_spec, qkv_spec, wout_spec, up_spec, down_spec), check_vma=False)
```

```python
import jax
import jax.numpy as jnp
from jax import lax
from jax.experimental import pallas as pl
from jax.sharding import PartitionSpec as P


MICROBATCHES = 2
LOG2E = 1.4426950408889634
F32 = jnp.float32
BF16 = jnp.bfloat16


def dot_f32(lhs, rhs, lhs_dim, rhs_dim):
    return lax.dot_general(lhs, rhs, (((lhs_dim,), (rhs_dim,)), ((), ())), preferred_element_type=F32)


def attention_body(heads_per_step, scale_factor, q_ref, k_ref, v_ref, datt_ref, out_ref, dqkv_ref):
    for head in range(heads_per_step):
        queries = q_ref[0, head]
        keys_all = k_ref[0, head]
        values = v_ref[0, head]
        d_att = datt_ref[0, head]
        scores = dot_f32(keys_all.T, queries, 1, 0)
        exps = jnp.exp2((scores - jnp.max(scores, axis=0, keepdims=True)) * (scale_factor * LOG2E))
        probs_f = exps * (1.0 / jnp.sum(exps, axis=0, keepdims=True))
        probs_b = probs_f.astype(BF16)
        out_ref[0, head] = dot_f32(values, probs_b, 1, 0).astype(BF16)
        d_probs = dot_f32(values.T, d_att, 1, 0)
        dqkv_ref[0, 2, head] = dot_f32(d_att, probs_b, 1, 1).astype(BF16)
        row_dot = jnp.sum(d_probs * probs_f, axis=0, keepdims=True)
        d_scores = (probs_f * (d_probs - row_dot) * scale_factor).astype(BF16)
        dqkv_ref[0, 0, head] = dot_f32(keys_all, d_scores, 1, 0).astype(BF16)
        dqkv_ref[0, 1, head] = dot_f32(queries, d_scores, 1, 1).astype(BF16)


def attention_backward(q_t, k_t, v_t, datt_t):
    batch, heads, head_dim, seq = datt_t.shape
    step = 2 if heads % 2 == 0 else 1
    flops = 12 * batch * heads * head_dim * seq * seq * 4

    def body(*refs):
        attention_body(step, head_dim ** -0.5, *refs)

    qkv_spec = pl.BlockSpec((1, 3, step, head_dim, seq), lambda b, n: (b, 0, n, 0, 0))
    att_spec = pl.BlockSpec((1, step, head_dim, seq), lambda b, n: (b, n, 0, 0))
    return pl.pallas_call(
        body,
        grid=(batch, heads // step),
        in_specs=[att_spec] * 4,
        out_specs=[att_spec, qkv_spec],
        out_shape=[jax.ShapeDtypeStruct(datt_t.shape, BF16), jax.ShapeDtypeStruct((batch, 3, heads, head_dim, seq), BF16)],
        cost_estimate=pl.CostEstimate(flops=flops, bytes_accessed=16 * datt_t.size, transcendentals=batch * heads * seq * seq),
        name='attn_bwd',
    )(q_t, k_t, v_t, datt_t)


def solution(mesh):
    data_axes = ('dpy', 'dpx')
    replicas = mesh.shape['dpy'] * mesh.shape['dpx']
    act_spec = P(None, data_axes, None, None)
    tok_spec = P(data_axes, None, None)
    qkv_spec = P(None, None, None, 'tp', None)
    wout_spec = P(None, 'tp', None, None)
    up_spec = P(None, None, 'tp')
    down_spec = P(None, 'tp', None)
    tp_size = mesh.shape['tp']
    core_swap = [(i, i ^ 1) for i in range(tp_size)]
    chip_swap = [(i, i ^ 2) for i in range(tp_size)]
    pair_swap = [(0, 1), (1, 0)]

    def after(values, *earlier):
        tied = lax.optimization_barrier((tuple(values), tuple(earlier)))
        return tied[0]

    def tp_sum_half(part, residual, offset, *earlier):
        core = lax.rem(lax.axis_index('tp'), 2)
        half = part.shape[0] // 2
        res_half = lax.dynamic_slice_in_dim(residual, offset + core * half, half, 0)
        from_core = lax.ppermute(lax.dynamic_slice_in_dim(part, (1 - core) * half, half, 0), 'tp', core_swap)
        own = lax.dynamic_slice_in_dim(part, core * half, half, 0)
        chip_sum = (own.astype(F32) + from_core.astype(F32)).astype(BF16)
        from_chip = lax.ppermute(chip_sum, 'tp', chip_swap)
        from_chip, = after((from_chip,), *earlier)
        mine = (res_half.astype(F32) + (chip_sum.astype(F32) + from_chip.astype(F32))).astype(BF16)
        return mine, lax.ppermute(mine, 'tp', core_swap), chip_sum

    def join_halves(mine, other, _):
        core = lax.rem(lax.axis_index('tp'), 2)
        is_mine = (jnp.arange(2) == core)[:, None, None, None]
        both = jnp.where(is_mine, mine[None], other[None])
        return both.reshape((2 * mine.shape[0],) + mine.shape[1:])

    class ReplicaMean:
        def __init__(self, grad):
            self.rows, self.cols = grad.shape
            self.idx_y, self.idx_x = lax.axis_index('dpy'), lax.axis_index('dpx')
            self.blocks = grad.reshape(2, 2, 2, self.rows // 8, self.cols)
            self.sends = (self.cut(0, 1 - self.idx_x, 0, 2, 1).astype(BF16), self.cut(1 - self.idx_y, 0, 1, 1, 2).astype(BF16))
            self.recvs = (lax.ppermute(self.sends[0], 'dpx', pair_swap), lax.ppermute(self.sends[1], 'dpy', pair_swap))

        def cut(self, pos_y, pos_x, half, size_y, size_x):
            size = self.rows // 8
            out = lax.dynamic_slice(self.blocks, (pos_y, pos_x, half, 0, 0), (size_y, size_x, 1, size, self.cols))
            return out.reshape(size_y * size_x * size, self.cols)

        def part(self, recv, index):
            size = self.rows // 8
            return lax.dynamic_slice_in_dim(recv, index * size, size, 0).astype(F32)

        def second(self, *earlier):
            idx_y, idx_x = self.idx_y, self.idx_x
            recvs = self.recvs = after(self.recvs, *earlier)
            self.sends = ((self.cut(1 - idx_y, idx_x, 0, 1, 1) + self.part(recvs[0], 1 - idx_y)).astype(BF16),
                          (self.cut(idx_y, 1 - idx_x, 1, 1, 1) + self.part(recvs[1], 1 - idx_x)).astype(BF16))
            self.lasts = (lax.ppermute(self.sends[0], 'dpy', pair_swap), lax.ppermute(self.sends[1], 'dpx', pair_swap))
            return self.sends

        def third(self, *earlier):
            idx_y, idx_x = self.idx_y, self.idx_x
            lasts = after(self.lasts, *earlier)
            sum_first = self.cut(idx_y, idx_x, 0, 1, 1) + self.part(self.recvs[0], idx_y) + lasts[0].astype(F32)
            sum_second = self.cut(idx_y, idx_x, 1, 1, 1) + self.part(self.recvs[1], idx_x) + lasts[1].astype(F32)
            self.mine = (jnp.concatenate([sum_first, sum_second], axis=0) / replicas).astype(BF16)
            return self.mine

        def gathered(self):
            return lax.all_gather(self.mine, data_axes, axis=0, tiled=True).astype(F32)

    def device_backward(x_saved, y_saved, d_out, w_qkv, w_out, w_up, w_down):
        num_layers, width, _, heads, head_dim = w_qkv.shape
        cols = heads * head_dim
        rows = d_out.shape[0] // MICROBATCHES
        seq = d_out.shape[1]
        micro = [slice(i * rows, (i + 1) * rows) for i in range(MICROBATCHES)]
        grads = [d_out[m] for m in micro]
        sources = [(d_out, i * rows) for i in range(MICROBATCHES)]
        outs = [None] * 4
        pending = []
        upper = {}

        def mlp_down(hidden, grad):
            return jnp.einsum('bsf,bsh->fh', jax.nn.gelu(hidden).astype(BF16), grad, preferred_element_type=F32)

        def place(layer, slots, means):
            for slot, mean in zip(slots, means):
                block = mean.gathered()[None]
                if layer == num_layers - 1:
                    edge = ((0, 0, 0), (0, 0, 0))
                    outs[slot] = lax.pad(block, jnp.zeros((), F32), ((layer, 0, 0), *edge))
                else:
                    outs[slot] = lax.dynamic_update_slice(outs[slot], block, (layer, 0, 0))

        def mlp_data(layer, hidden, grad):
            _, gelu_pull = jax.vjp(jax.nn.gelu, hidden)
            d_act = jnp.einsum('bsh,fh->bsf', grad, w_down[layer], preferred_element_type=F32)
            d_hidden = gelu_pull(d_act)[0].astype(BF16)
            return d_hidden, jnp.einsum('bsf,hf->bsh', d_hidden, w_up[layer], preferred_element_type=F32).astype(BF16)

        for layer in reversed(range(num_layers)):
            wqkv_t = w_qkv[layer].transpose(1, 2, 3, 0).reshape(3 * cols, width)
            wout_l = w_out[layer].reshape(cols, width)
            hid = [jnp.einsum('bsh,hf->bsf', y_saved[layer, m], w_up[layer], preferred_element_type=F32) for m in micro]
            g_down = mlp_down(hid[0], grads[0])
            sends = [s for mean in pending for s in mean.second(g_down)]
            g_down = g_down + mlp_down(after((hid[1],), g_down, *sends)[0], grads[1])
            edges = [mean.third(g_down) for mean in pending]
            down = ReplicaMean(g_down)
            if layer < num_layers - 1:
                place(layer + 1, (2, 3), upper['mlp'])
                tied = after((hid[0], *outs[2:]), *down.sends, *edges)
                hid_0, outs[2:] = tied[0], tied[1:]
            else:
                hid_0, = after((hid[0],), *down.sends)
            d_hid_0, mid_0 = mlp_data(layer, hid_0, grads[0])
            mid_halves = [tp_sum_half(mid_0, *sources[0])]
            sends = down.second(mid_0)
            d_hid_1, mid_1 = mlp_data(layer, after((hid[1],), mid_0, mid_halves[0][2], *sends)[0], grads[1])
            mid_halves.append(tp_sum_half(mid_1, *sources[1], mid_halves[0][0]))
            mine = down.third(mid_1)
            d_hid_0, = after((d_hid_0,), mid_1, mine)
            g_up = jnp.einsum('bsh,bsf->hf', y_saved[layer, micro[0]], d_hid_0, preferred_element_type=F32)
            d_hid_1, = after((d_hid_1,), g_up, mid_halves[1][2])
            g_up += jnp.einsum('bsh,bsf->hf', y_saved[layer, micro[1]], d_hid_1, preferred_element_type=F32)
            up = ReplicaMean(g_up)
            edges = list(up.sends)
            if layer < num_layers - 1:
                place(layer + 1, (0, 1), upper['att'])
            mids, halves, out_ts, dqkv_ts = [], [], [], []
            for i, m in enumerate(micro):
                x_in = x_saved[layer, m]
                d_mid = join_halves(*after(mid_halves[i], *edges))
                if i == 0 and layer < num_layers - 1:
                    d_mid, *outs[:2] = after((d_mid, *outs[:2]))
                else:
                    d_mid, = after((d_mid,))
                qkv_t = [jnp.einsum('hnd,bsh->bnds', w_qkv[layer, :, c], x_in, preferred_element_type=F32).astype(BF16) for c in range(3)]
                datt_t = jnp.einsum('jh,bsh->bjs', wout_l, d_mid, preferred_element_type=F32).astype(BF16)
                out_t, dqkv_t = attention_backward(*[t.reshape(rows, heads, head_dim, seq) for t in (*qkv_t, datt_t)])
                dqkv_t = dqkv_t.reshape(rows, 3 * cols, seq)
                if i == 0:
                    sends = up.second(out_t)
                    dqkv_t, = after((dqkv_t,), *sends)
                elif layer == 0:
                    dqkv_t, g_qkv = after((dqkv_t, g_qkv))
                    g_qkv += jnp.einsum('bjs,bsh->jh', dqkv_t, x_in, preferred_element_type=F32)
                    qkv_mean = ReplicaMean(g_qkv)
                    dqkv_t, = after((dqkv_t,), *qkv_mean.sends)
                in_part = jnp.einsum('bjs,jh->bsh', dqkv_t, wqkv_t, preferred_element_type=F32).astype(BF16)
                halves.append(tp_sum_half(in_part, d_mid, 0, *[half[0] for half in halves]))
                if i == 0:
                    edges = [in_part, halves[0][2], up.third(in_part)]
                    if layer == 0:
                        g_qkv = jnp.einsum('bjs,bsh->jh', after((dqkv_t,), in_part)[0], x_in, preferred_element_type=F32)
                        edges.append(g_qkv)
                mids.append(d_mid)
                out_ts.append(out_t.reshape(rows, cols, seq))
                dqkv_ts.append(dqkv_t)
            if layer > 0:
                dqkv_0, = after((dqkv_ts[0],), in_part)
                g_qkv = jnp.einsum('bjs,bsh->jh', dqkv_0, x_saved[layer, micro[0]], preferred_element_type=F32)
                dqkv_1, = after((dqkv_ts[1],), g_qkv, halves[1][2])
                g_qkv += jnp.einsum('bjs,bsh->jh', dqkv_1, x_saved[layer, micro[1]], preferred_element_type=F32)
                qkv_mean = ReplicaMean(g_qkv)
            out_ts = after(out_ts, in_part, halves[1][2], *qkv_mean.sends)
            g_out = sum(jnp.einsum('bjs,bsh->jh', out_ts[i], mids[i], preferred_element_type=F32) for i in range(MICROBATCHES))
            out_mean = ReplicaMean(g_out)
            upper = {'mlp': (up, down), 'att': (qkv_mean, out_mean)}
            if layer > 0:
                pending = [qkv_mean, out_mean]
                grad_0, = after((join_halves(*after(halves[0], in_part)),), *qkv_mean.sends, *out_mean.sends)
                grads = [grad_0, after((join_halves(*after(halves[1], grad_0)),))[0]]
                sources = [(g, 0) for g in grads]
        place(0, (2, 3), upper['mlp'])
        outs[2:] = after(outs[2:])
        for mean in upper['att']:
            mean.second(outs[2])
            mean.third()
        place(0, (0, 1), upper['att'])
        core = lax.rem(lax.axis_index('tp'), 2)
        d_in = lax.pad(join_halves(*after(halves[0], in_part)), jnp.zeros((), BF16), ((0, rows, 0), (0, 0, 0), (0, 0, 0)))
        mine, other, _ = halves[1]
        half = mine.shape[0]
        d_in = lax.dynamic_update_slice_in_dim(d_in, mine, rows + core * half, 0)
        d_in = lax.dynamic_update_slice_in_dim(d_in, other, rows + (1 - core) * half, 0)
        g_qkv = outs[0].reshape(num_layers, 3, heads, head_dim, width).transpose(0, 4, 1, 2, 3)
        g_out = outs[1].reshape(num_layers, heads, head_dim, width)
        return d_in, g_qkv, g_out, outs[2], outs[3]

    return jax.shard_map(device_backward, mesh=mesh, in_specs=(act_spec, act_spec, tok_spec, qkv_spec, wout_spec, up_spec, down_spec), out_specs=(tok_spec, qkv_spec, wout_spec, up_spec, down_spec), check_vma=False)
```
